32 devices in a mesh: ep: 4 (over x, core), tp: 8 (over z, y).
Axes of the slice: x: 2, y: 2, z: 4, core: 2. Of those that a mesh axis runs over, the one named last changes fastest.
Arguments:
- layer_input: bfloat16 [1024, 4096], P('ep', 'tp'), may hold values from -6 to 6
- out_grad: bfloat16 [1024, 4096], P('ep', 'tp'), may hold values from -6 to 6
- route: int32 [1024, 2], P('ep'), may hold values from 0 to 3, all different within a row; in each aligned block of 256 rows (0 to 255, 256 to 511, ...) at most 192 rows name the same one
- gate_share: float32 [1024, 2], P('ep'), may hold values from 0.2 to 1
- gate_weight: bfloat16 [4, 4096, 14336], P('ep', None, 'tp'), may hold values from -0.125 to 0.125
- up_weight: bfloat16 [4, 4096, 14336], P('ep', None, 'tp'), may hold values from -0.125 to 0.125
- down_weight: bfloat16 [4, 14336, 4096], P('ep', 'tp'), may hold values from -0.046875 to 0.046875
Outputs:
- input_grad: bfloat16 [1024, 4096], P('ep', 'tp')
The draws below stay inside these ranges and needn't reach their ends.
Inputs may be any that keep to these rules, and one draw needn't show every extreme that they name: `route`: each row names 2 different experts. In each aligned block of 256 rows (the rows of one index of ep) no expert is named by more than 192 rows, a bound that some block reaches.
All inputs are finite; a program needn't handle non-finite values.
Results may differ from the reference program's by a relative error of at most 0.0057.
Values may be sent and summed in bfloat16 or wider, within the bound.
A program may use at most 320 MiB of HBM per device.

```python
import math
import jax
import jax.numpy as jnp
import numpy as np
from jax import lax

D = 4096
FF = 14336
TOP = 2
TOK_EP = 256
EXPERTS = 4
CAP = 192
TOKENS = 1024
N_EP = 4


def with_spikes(result, rng, source, target, blocks, factor):
    def block_of(dim):
        return (jnp.arange(result.shape[dim]) // (result.shape[dim] // blocks)).reshape((-1,) + (1,) * (result.ndim - 1 - dim))

    first = jax.random.permutation(rng, blocks)[block_of(target)]
    second = (block_of(target) + blocks // 2) % blocks
    return jnp.where((block_of(source) == first) | (block_of(source) == second), factor * result, result)


def shard_levels(key, extent, shards, low, high):
    loudness = 1.0
    for dim, blocks in shards:
        heights = jax.random.uniform(jax.random.fold_in(jax.random.fold_in(key, 6), dim), (blocks,), jnp.float32, low / len(shards), high / len(shards))
        loudness = loudness * jnp.repeat(jnp.exp(heights), extent[dim] // blocks).reshape((-1,) + (1,) * (len(extent) - 1 - dim))
    return loudness


def deal_out(rng, own, number, rows, count, top, most, lean):
    sequence = jax.random.permutation(rng, count)
    heavy_load, common = portions_of(count, rows * top, most, lean, True), portions_of(count, rows * top, most, lean, False)
    places = jnp.arange(count)

    def named(tallies, turn):
        used = int((tallies > 0).sum())
        fixed = max(1, used // 4)
        shifted = fixed + (places - fixed + turn * (used - fixed)) % max(1, count - fixed)
        return jnp.zeros((count,), jnp.int32).at[sequence[jnp.where(places < fixed, places, shifted)]].set(jnp.asarray(tallies, jnp.int32))

    tallies = jnp.where(number % 4 == 0, named(heavy_load, number // 4), named(common, number - number // 4 - 1))
    mixed = jax.random.permutation(jax.random.fold_in(own, 3), count)
    donor, receiver = mixed[0:count // 2 * 2:2], mixed[1:count // 2 * 2:2]
    margin = jnp.minimum(tallies[donor] - 1, most - tallies[receiver]) // 2
    margin = jnp.where((donor == sequence[0]) | (receiver == sequence[0]) | (tallies[receiver] == 0), 0, jnp.maximum(margin, 0))
    shifted = jax.random.randint(jax.random.fold_in(own, 4), (count // 2,), 0, 1 << 20) % (margin + 1)
    tallies = tallies.at[donor].add(-shifted).at[receiver].add(shifted)
    items = jnp.searchsorted(jnp.cumsum(tallies), jnp.arange(rows * top), side="right").astype(jnp.int32)
    grid = items.reshape(top, rows).T
    grid = grid[jax.random.permutation(jax.random.fold_in(own, 1), rows)]
    turn = jax.random.randint(jax.random.fold_in(own, 2), (rows, 1), 0, top)
    return jnp.take_along_axis(grid, (jnp.arange(top)[None, :] + turn) % top, axis=1)


def portions_of(count, total, most, lean, full):
    loads = [(1 << 20) // math.isqrt(standing ** lean) + 1 for standing in range(1, count + 1)]
    largest = most if full else min(most, max(-(-total // count), total * loads[0] // sum(loads)))
    least = 1 if total - largest >= count - 1 else 0
    holding, spare = [largest] + [least] * (count - 1), total - largest - least * (count - 1)
    while spare > 0:
        free = [i for i in range(1, count) if holding[i] < largest] or [i for i in range(1, count) if holding[i] < most]
        whole, budget = sum([loads[i] for i in free]), spare
        for i in free:
            addition = min(most - holding[i], max(1, budget * loads[i] // whole), spare)
            holding[i] = holding[i] + addition
            spare = spare - addition
    return np.array(holding)


def centred(stream_key, shape, width, limit, split=(), held_as=jnp.bfloat16):
    values = width * jax.random.normal(stream_key, shape, jnp.float32)
    if split:
        values = values * shard_levels(stream_key, shape, split, -0.22, 0.18)
    return jnp.clip(values, -limit, limit).astype(held_as)


def gaussian_with(stream_key, shape, deviation, limit, pieces, heavy, kind=jnp.bfloat16):
    values = deviation * jax.random.normal(stream_key, shape, jnp.float32)
    if pieces:
        values = values * shard_levels(stream_key, shape, pieces, -0.22, 0.18)
    return jnp.clip(with_spikes(values, jax.random.fold_in(stream_key, 3), *heavy), -limit, limit).astype(kind)


def setup_inputs(seed: int = 0) -> dict:
    seeds = jax.random.split(jax.random.key(seed), 8)
    layer_input = centred(seeds[0], (TOKENS, D), 1.0, 6.0, ((0, 4), (1, 8)))
    out_grad = centred(seeds[1], (TOKENS, D), 1.0, 6.0, ((0, 4), (1, 8)))
    route_keys = jax.random.split(jax.random.fold_in(seeds[2], 1), TOKENS // TOK_EP)
    route_turns = jax.random.permutation(jax.random.fold_in(seeds[2], 3), TOKENS // TOK_EP)
    route = jax.vmap(lambda own, number: deal_out(jax.random.fold_in(seeds[2], 2), own, number, TOK_EP, EXPERTS, TOP, CAP, 2))(route_keys, route_turns).reshape((TOKENS, TOP))
    gate_share = jnp.clip(0.2 + 0.8 * jax.random.uniform(seeds[3], (TOKENS, TOP), jnp.float32) ** shard_levels(seeds[3], (TOKENS, TOP), ((0, 4),), -0.2, 0.2), 0.2, 1.0)
    gate_weight = gaussian_with(seeds[4], (EXPERTS, D, FF), D ** -0.5, 0.125, ((0, 4), (2, 8)), (2, 1, 8, 2.0))
    up_weight = gaussian_with(seeds[5], (EXPERTS, D, FF), D ** -0.5, 0.125, ((0, 4), (2, 8)), (2, 1, 8, 2.0))
    down_weight = centred(seeds[6], (EXPERTS, FF, D), FF ** -0.5, 0.046875, ((0, 4), (1, 8)))
    return {"layer_input": layer_input, "out_grad": out_grad, "route": route, "gate_share": gate_share, "gate_weight": gate_weight, "up_weight": up_weight, "down_weight": down_weight}


def slot_positions(blocks):
    onehot = (blocks[..., None] == jnp.arange(EXPERTS, dtype=jnp.int32)).astype(jnp.int32).sum(axis=2)
    before = jnp.cumsum(onehot, axis=1) - onehot
    return jnp.take_along_axis(before, blocks, axis=2).astype(jnp.int32)


def expert_rows(gate_matrix, up_matrix, down_matrix, inputs, grads):
    gate_act = jnp.dot(inputs, gate_matrix, preferred_element_type=jnp.float32)
    up_act = jnp.dot(inputs, up_matrix, preferred_element_type=jnp.float32)
    hidden_grad = lax.dot_general(grads, down_matrix, (((1,), (1,)), ((), ())), preferred_element_type=jnp.float32)
    sigma = jax.nn.sigmoid(gate_act)
    slope = sigma * (1.0 + gate_act * (1.0 - sigma))
    gate_grad = (hidden_grad * up_act * slope).astype(jnp.bfloat16)
    up_grad = (hidden_grad * gate_act * sigma).astype(jnp.bfloat16)
    total = lax.dot_general(gate_grad, gate_matrix, (((1,), (1,)), ((), ())), preferred_element_type=jnp.float32)
    total = total + lax.dot_general(up_grad, up_matrix, (((1,), (1,)), ((), ())), preferred_element_type=jnp.float32)
    return total.astype(jnp.bfloat16)


def reference(layer_input, out_grad, route, gate_share, gate_weight, up_weight, down_weight):
    blocks = route.reshape(N_EP, TOK_EP, TOP)
    position = slot_positions(blocks)
    flat = blocks * CAP + position
    owner = jnp.broadcast_to(jnp.arange(TOK_EP, dtype=jnp.int32)[None, :, None], flat.shape)
    block_index = jnp.broadcast_to(jnp.arange(N_EP, dtype=jnp.int32)[:, None, None], flat.shape)
    inverse = jnp.full((N_EP, EXPERTS * CAP), TOK_EP, jnp.int32)
    inverse = inverse.at[block_index.reshape(-1), flat.reshape(-1)].set(owner.reshape(-1))
    inverse = inverse.reshape(N_EP, EXPERTS, CAP)

    def one_expert(expert):
        local = lax.dynamic_index_in_dim(inverse, expert, 1, keepdims=False)
        valid = (local < TOK_EP).reshape(-1)[:, None]
        rows = (jnp.arange(N_EP, dtype=jnp.int32)[:, None] * TOK_EP + jnp.minimum(local, TOK_EP - 1)).reshape(-1)
        zero_value = jnp.zeros((), layer_input.dtype)
        inputs = jnp.where(valid, jnp.take(layer_input, rows, axis=0), zero_value)
        grads = jnp.where(valid, jnp.take(out_grad, rows, axis=0), zero_value)
        gate_matrix = lax.dynamic_index_in_dim(gate_weight, expert, 0, keepdims=False)
        up_matrix = lax.dynamic_index_in_dim(up_weight, expert, 0, keepdims=False)
        down_matrix = lax.dynamic_index_in_dim(down_weight, expert, 0, keepdims=False)
        return expert_rows(gate_matrix, up_matrix, down_matrix, inputs, grads)

    returned = lax.map(one_expert, jnp.arange(EXPERTS, dtype=jnp.int32))
    returned = returned.reshape(EXPERTS, N_EP, CAP, D)
    picked = returned[blocks, block_index, position]
    shares = gate_share.reshape(N_EP, TOK_EP, TOP)[..., None]
    combined = jnp.sum(picked.astype(jnp.float32) * shares, axis=2)
    return combined.reshape(TOKENS, D).astype(jnp.bfloat16)
```

```python
import jax
import jax.numpy as jnp
from jax import lax
from jax.sharding import PartitionSpec as P

CORES = 2


def local(layer_input, out_grad, route, gate_share, gate_weight, up_weight, down_weight):
    groups = lax.axis_size("ep")
    me = lax.axis_index("ep")
    chips = groups // CORES
    rows = layer_input.shape[0]
    gate_matrix = gate_weight[0]
    up_matrix = up_weight[0]
    down_matrix = down_weight[0]

    def shift(value, step):
        pairs = [(i, (i + step * CORES) % groups) for i in range(groups)]
        return lax.ppermute(value, "ep", pairs)

    def swap(value):
        return lax.ppermute(value, "ep", [(i, i ^ 1) for i in range(groups)])

    members = lax.axis_size("tp")
    inner = 1
    while 4 * inner * inner <= members:
        inner *= 2
    outer = members // inner
    place = lax.axis_index("tp")
    place_outer, place_inner = place // inner, place % inner
    width = layer_input.shape[1]

    def turn(value, outer_step, inner_step):
        pairs = []
        for i in range(members):
            target = (i // inner + outer_step) % outer * inner + (i % inner + inner_step) % inner
            pairs.append((i, target))
        return lax.ppermute(value, "tp", pairs)

    def gather(value):
        line = jnp.stack([value] + [turn(value, a, 0) for a in range(1, outer)])
        return jnp.concatenate([line] + [turn(line, 0, b) for b in range(1, inner)])

    def in_order(blocks):
        both = jnp.concatenate([blocks, swap(blocks)], axis=1)
        full = jnp.zeros((both.shape[1], members * width), both.dtype)
        for b in range(inner):
            for a in range(outer):
                source = (place_outer - a) % outer * inner + (place_inner - b) % inner
                full = lax.dynamic_update_slice(full, both[b * outer + a], (0, source * width))
        return full

    def scatter(value):
        def blocks_for(b):
            owner = (place_inner + b) % inner
            return [
                lax.dynamic_slice_in_dim(
                    value, ((place_outer + a) % outer * inner + owner) * width, width, axis=1
                )
                for a in range(outer)
            ]

        lines = jnp.stack(blocks_for(0))
        for b in range(1, inner):
            sent = jnp.stack(blocks_for(b)).astype(jnp.bfloat16)
            lines = lines + turn(sent, 0, b).astype(jnp.float32)
        result = lines[0]
        for a in range(1, outer):
            sent = turn(lines[a].astype(jnp.bfloat16), a, 0)
            result = result + sent.astype(jnp.float32)
        return result

    experts = jnp.arange(groups, dtype=jnp.int32)
    shares = jnp.sum(
        jnp.where(route[:, :, None] == experts, gate_share[:, :, None], 0.0), axis=1
    )

    gathered = []
    for step in range(chips):
        if step:
            part_input, part_grad = shift(layer_input, step), shift(out_grad, step)
            part_share = shift(shares, step)
        else:
            part_input, part_grad, part_share = layer_input, out_grad, shares
        full_input = gather(part_input)
        full_grad = gather(part_grad)
        share = jnp.concatenate([part_share, swap(part_share)], axis=0)
        share = jnp.sum(jnp.where(experts == me, share, 0.0), axis=1, keepdims=True)
        gathered.append((full_input, full_grad, share))

    total = None
    for step in range(chips):
        full_input, full_grad, share = gathered[step]
        inputs = in_order(full_input)
        grads = in_order(full_grad)
        gate_sum = jnp.dot(inputs, gate_matrix, preferred_element_type=jnp.float32)
        up_sum = jnp.dot(inputs, up_matrix, preferred_element_type=jnp.float32)
        hidden_sum = lax.dot_general(
            grads, down_matrix, (((1,), (1,)), ((), ())), preferred_element_type=jnp.float32
        )
        sigma = jax.nn.sigmoid(gate_sum)
        slope = sigma * (1.0 + gate_sum * (1.0 - sigma))
        gate_grad = (hidden_sum * up_sum * slope).astype(jnp.bfloat16)
        up_grad = (hidden_sum * gate_sum * sigma).astype(jnp.bfloat16)
        partial = lax.dot_general(
            gate_grad, gate_matrix, (((1,), (1,)), ((), ())), preferred_element_type=jnp.float32
        )
        partial = partial + lax.dot_general(
            up_grad, up_matrix, (((1,), (1,)), ((), ())), preferred_element_type=jnp.float32
        )
        partial = jnp.where(share > 0.0, partial * share, 0.0)
        other = swap(partial[rows:].astype(jnp.bfloat16))
        summed = scatter(partial[:rows] + other.astype(jnp.float32))
        if step:
            summed = shift(summed.astype(jnp.bfloat16), chips - step).astype(jnp.float32)
        total = summed if total is None else total + summed
    return total.astype(jnp.bfloat16)


def solution(mesh):
    return jax.shard_map(
        local,
        mesh=mesh,
        in_specs=(
            P("ep", "tp"),
            P("ep", "tp"),
            P("ep", None),
            P("ep", None),
            P("ep", None, "tp"),
            P("ep", None, "tp"),
            P("ep", "tp", None),
        ),
        out_specs=P("ep", "tp"),
        check_vma=False,
    )
```
